128 devices in a mesh: freq: 64 (over x, y, z_hi, core), depth: 2 (over z_lo).
Axes of the slice: x: 4, y: 4, z: 4 (z_hi: 2, z_lo: 2; z = z_hi * 2 + z_lo), core: 2. Of those that a mesh axis runs over, the one named last changes fastest.
Arguments:
- pressure_field: bfloat16 [8192, 16384], P('depth', 'freq'), may hold values from -6 to 6
- block_main: bfloat16 [8192, 3, 2, 128], P('depth'), may hold values from -0.15625 to 0.15625
- block_coupled: bfloat16 [8192, 3, 2, 128], P('depth'), may hold values from -0.15625 to 0.15625
- coupling: float32 [16384], P('freq'), may hold values from -3 to 3
- frequencies: float32 [8192], replicated, may hold values from 1 to 1024
- receivers: int32 [512], replicated, may hold values from 0 to 8191
- floors: int32 [4], replicated, may hold values from 2048 to 8191
Outputs:
- series: float32 [512, 2048], P('depth', 'freq')
The draws below stay inside these ranges and needn't reach their ends.
Inputs may be any that keep to these rules, and one draw needn't show every extreme that they name: `receivers`: any depth cells, repeats possible.
All inputs are finite; a program needn't handle non-finite values.
Results may differ from the reference program's by a relative error of at most 0.0061.
Values may be sent and summed in bfloat16 or wider, within the bound.
No kernel may reach another device: no remote copies, remote signals or barrier semaphores. Data moves between devices by JAX's collectives and lax.ppermute only.
A program may use at most 256 MiB of HBM per device.

```python
import math
import jax
import jax.numpy as jnp
from jax import lax

NZ = 8192
BS = 128
NT = 2048
R = 512
STEPS = 4
F_DEV = 128
F = 8192
N_FREQ = 64


def touch_ends(array, key, smallest, largest):
    index_at = [jax.random.randint(jax.random.fold_in(key, axis), (), 0, length) for axis, length in enumerate(array.shape)]
    main_axis = array.shape.index(max(array.shape))
    next_to = index_at[:main_axis] + [(index_at[main_axis] + 1) % array.shape[main_axis]] + index_at[main_axis + 1:]
    return array.at[tuple(index_at)].set(smallest).at[tuple(next_to)].set(largest)


def levels(own_key, shape, cuts, least, top_value):
    level = 1.0
    for position, blocks in cuts:
        draws = jax.random.uniform(jax.random.fold_in(jax.random.fold_in(own_key, 6), position), (blocks,), jnp.float32, least / len(cuts), top_value / len(cuts))
        level = level * jnp.repeat(jnp.exp(draws), shape[position] // blocks).reshape((-1,) + (1,) * (len(shape) - 1 - position))
    return level


def gaussian(stream_key, dims, scale, reach, split=(), held_as=jnp.bfloat16):
    entries = scale * jax.random.normal(stream_key, dims, jnp.float32)
    if split:
        entries = entries * levels(stream_key, dims, split, -0.22, 0.18)
    return jnp.clip(entries, -reach, reach).astype(held_as)


def setup_inputs(seed: int = 0) -> dict:
    streams_of = jax.random.split(jax.random.key(seed), 8)
    return {
        "pressure_field": gaussian(streams_of[0], (NZ, 2 * F), 1.0, 6.0, ((0, 2), (1, 64))),
        "block_main": gaussian(streams_of[1], (NZ, 3, 2, BS), (12 * BS) ** -0.5, 0.15625, ((0, 2),)),
        "block_coupled": gaussian(streams_of[2], (NZ, 3, 2, BS), (12 * BS) ** -0.5, 0.15625, ((0, 2),)),
        "coupling": gaussian(streams_of[3], (2 * F,), 0.5, 3.0, ((0, 64),), jnp.float32),
        "frequencies": jnp.clip(jax.random.uniform(streams_of[4], (F,), jnp.float32, 1.0, 1024.0), 1.0, 1024.0),
        "receivers": touch_ends(jax.random.randint(streams_of[5], (R,), 0, NZ), jax.random.fold_in(streams_of[5], 1), 0, NZ - 1).astype(jnp.int32),
        "floors": touch_ends(jax.random.randint(streams_of[6], (STEPS,), NZ // 4, NZ), jax.random.fold_in(streams_of[6], 1), NZ // 4, NZ - 1).astype(jnp.int32),
    }


def apply_blocks(blocks, padded):
    block_count = blocks.shape[0]
    width = padded.shape[1]
    stacked = padded.reshape(block_count + 2, BS, width)
    neighbours = jnp.stack([stacked[:-2], stacked[1:-1], stacked[2:]], axis=1)
    product = jnp.einsum('bikrj,bkjc->rbic', blocks, neighbours, precision=lax.Precision.HIGHEST)
    real_part = product[0].reshape(block_count * BS, width)
    imag_part = product[1].reshape(block_count * BS, width // 2, 2)
    rotated = jnp.stack([-imag_part[..., 1], imag_part[..., 0]], axis=-1).reshape(block_count * BS, width)
    return real_part + rotated

def couple_terms(values, weights):
    height = values.shape[0]
    paired = values.reshape(height, -1, 2)
    wpair = weights.reshape(-1, 2)
    real_part = wpair[:, 0] * paired[..., 0] - wpair[:, 1] * paired[..., 1]
    imag_part = wpair[:, 0] * paired[..., 1] + wpair[:, 1] * paired[..., 0]
    return jnp.stack([real_part, imag_part], axis=-1).reshape(height, -1)

def make_basis(freq_values, sample_times):
    phase = jnp.mod(freq_values[:, None] * sample_times[None, :], jnp.float32(NT)) / jnp.float32(NT)
    angle = 2.0 * math.pi * phase
    stacked = jnp.stack([jnp.cos(angle), -jnp.sin(angle)], axis=1)
    return stacked.reshape(2 * freq_values.shape[0], sample_times.shape[0]).astype(jnp.bfloat16)

def reference(pressure_field, block_main, block_coupled, coupling, frequencies, receivers, floors):
    block_count = NZ // BS
    main_blocks = block_main.astype(jnp.float32).reshape(block_count, BS, 3, 2, BS)
    side_blocks = block_coupled.astype(jnp.float32).reshape(block_count, BS, 3, 2, BS)
    grouped = pressure_field.reshape(NZ, N_FREQ, 2 * F_DEV).transpose(1, 0, 2)
    pairs = coupling.reshape(N_FREQ, 2 * F_DEV)
    freq_groups = frequencies.reshape(N_FREQ, F_DEV)
    depth_index = jnp.arange(NZ, dtype=jnp.int32)
    sample_times = jnp.arange(NT, dtype=jnp.float32)

    def one_group(running, group_items):
        columns, weights, freq_values = group_items
        for step in range(STEPS):
            padded = jnp.pad(columns.astype(jnp.float32), ((BS, BS), (0, 0)))
            combined = apply_blocks(main_blocks, padded) + couple_terms(apply_blocks(side_blocks, padded), weights)
            damping = jnp.where(depth_index >= floors[step], 0.5, 1.0).astype(jnp.float32)
            columns = (damping[:, None] * combined).astype(jnp.bfloat16)
        picked = jnp.take(columns, receivers, axis=0)
        basis_table = make_basis(freq_values, sample_times)
        return (running + jnp.dot(picked, basis_table, preferred_element_type=jnp.float32), None)
    running, _ = lax.scan(one_group, jnp.zeros((R, NT), jnp.float32), (grouped, pairs, freq_groups))
    return running * (1.0 / math.sqrt(F))
```

```python
import math

import jax
import jax.numpy as jnp
from jax import lax
from jax.experimental import pallas as pl
from jax.experimental.pallas import tpu as pltpu
from jax.sharding import Mesh, PartitionSpec as P

NT = 2048
STEPS = 4
BS = 128
F32 = jnp.float32
BF16 = jnp.bfloat16
CHUNKS = 8
UNROLL = 8

VMEM_SPEC = pl.BlockSpec(memory_space=pltpu.VMEM)
HBM_SPEC = pl.BlockSpec(memory_space=pl.ANY)
SMEM_SPEC = pl.BlockSpec(memory_space=pltpu.SMEM)


def limit(mebibytes):
    return pltpu.CompilerParams(vmem_limit_bytes=mebibytes << 20)


def in_hbm(x):
    return pltpu.with_memory_space_constraint(x, pltpu.HBM)


def vmem(shape, dtype):
    return pltpu.VMEM(shape, dtype)


def split_matrix(width):
    half = width // 2
    source = lax.broadcasted_iota(jnp.int32, (width, width), 0)
    target = lax.broadcasted_iota(jnp.int32, (width, width), 1)
    return jnp.where(source == 2 * (target % half) + target // half, 1.0, 0.0).astype(F32)


def put_block(ref, b, field):
    half = field.shape[1] // 2
    at = b * (2 * BS)
    if not isinstance(at, int):
        at = pl.multiple_of(at, 2 * BS)
    real = field[:, :half]
    imag = field[:, half:]
    ref[pl.ds(at, BS), :] = field
    ref[pl.ds(at + BS, BS), :half] = -imag
    ref[pl.ds(at + BS, BS), half:] = real


def advanced(ordered, stacked, weights, first_row, floor_row):
    product = jnp.dot(ordered, stacked, preferred_element_type=F32)
    size = product.shape[0] // 2
    half = product.shape[1] // 2
    wr = weights[0:1, :half]
    wi = weights[0:1, half:]
    side_real = product[size:, :half]
    side_imag = product[size:, half:]
    real = product[:size, :half] + (wr * side_real - wi * side_imag)
    imag = product[:size, half:] + (wr * side_imag + wi * side_real)
    row = first_row + lax.broadcasted_iota(jnp.int32, (size, half), 0)
    damping = jnp.where(row >= floor_row, 0.5, 1.0).astype(F32)
    return jnp.concatenate([damping * real, damping * imag], axis=1).astype(BF16)


def zero_ends(ref):
    edge = jnp.zeros((2 * BS, ref.shape[1]), ref.dtype)
    ref[0 : 2 * BS, :] = edge
    ref[ref.shape[0] - 2 * BS :, :] = edge


def first_step(
    main_hbm, side_hbm, field_hbm, coupling_hbm, floors_hbm,
    ordered_ref, start_ref, next_ref, weight_ref,
    main_buf, side_buf, field_buf, planes, coupling_buf, floors_buf, sems, small_sems,
):
    blocks = ordered_ref.shape[0]
    per = blocks // CHUNKS
    rows = per * BS
    op_rows = rows * 6
    width = field_buf.shape[1]
    coupling_copy = pltpu.make_async_copy(coupling_hbm, coupling_buf, small_sems.at[0])
    floors_copy = pltpu.make_async_copy(floors_hbm, floors_buf, small_sems.at[1])
    coupling_copy.start()
    floors_copy.start()
    copies = []
    for n in range(CHUNKS):
        copies.append(
            [
                pltpu.make_async_copy(
                    source.at[pl.ds(n * size, size), :], buf.at[pl.ds(n * size, size), :], sems.at[kind, n]
                )
                for kind, (source, buf, size) in enumerate(
                    ((field_hbm, field_buf, rows), (main_hbm, main_buf, op_rows), (side_hbm, side_buf, op_rows))
                )
            ]
        )
    copies[0][0].start()
    copies[1][0].start()
    for n in range(CHUNKS):
        copies[n][1].start()
        copies[n][2].start()
        if n + 2 < CHUNKS:
            copies[n + 2][0].start()
    perm = split_matrix(width)
    for ref in (start_ref, next_ref):
        zero_ends(ref)
    coupling_copy.wait()
    floors_copy.wait()
    weights = jnp.dot(
        jnp.broadcast_to(coupling_buf[...], (8, width)), perm, preferred_element_type=F32, precision=lax.Precision.HIGHEST
    )
    weight_ref[...] = weights
    perm = perm.astype(BF16)
    first_row = lax.axis_index("depth") * (blocks * BS)
    floor_row = floors_buf[0] - first_row

    def split_chunk(n):
        copies[n][0].wait()
        for j in range(per):
            b = n * per + j
            field = jnp.dot(field_buf[b * BS : (b + 1) * BS, :], perm, preferred_element_type=F32).astype(BF16)
            put_block(start_ref, b + 1, field)

    split_chunk(0)
    for n in range(CHUNKS):
        if n + 1 < CHUNKS:
            split_chunk(n + 1)
        copies[n][1].wait()
        copies[n][2].wait()
        for j in range(per):
            b = n * per + j
            for kind, buf in enumerate((main_buf, side_buf)):
                plane = planes.at[j * 2 + kind]
                plane[...] = buf[b * BS * 6 : (b + 1) * BS * 6, :].astype(F32)
                for m in range(6):
                    ordered_ref[b, kind * BS : (kind + 1) * BS, m * BS : (m + 1) * BS] = plane[
                        pl.ds(m, BS, stride=6), :
                    ].astype(BF16)
        for j in range(per):
            b = n * per + j
            stacked = start_ref[b * 2 * BS : (b + 3) * 2 * BS, :]
            put_block(next_ref, b + 1, advanced(ordered_ref[b], stacked, weights, b * BS, floor_row))


def whole_step(step, last):
    def kernel(ordered_ref, field_ref, weight_ref, floors_ref, next_ref):
        blocks = ordered_ref.shape[0]
        first_row = lax.axis_index("depth") * (blocks * BS)
        floor_row = floors_ref[step] - first_row
        weights = weight_ref[...]
        if last:
            next_ref[blocks * BS :, :] = jnp.zeros((next_ref.shape[0] - blocks * BS, next_ref.shape[1]), F32)
        else:
            zero_ends(next_ref)

        def some(n, carry):
            for j in range(UNROLL):
                b = n * UNROLL + j
                at = pl.multiple_of(b * BS, BS)
                stacked = field_ref[pl.ds(pl.multiple_of(at * 2, 2 * BS), 6 * BS), :]
                field = advanced(ordered_ref[b], stacked, weights, at, floor_row)
                if last:
                    next_ref[pl.ds(at, BS), :] = field.astype(F32)
                else:
                    put_block(next_ref, b + 1, field)
            return carry

        lax.fori_loop(0, blocks // UNROLL, some, 0)

    return kernel


def edge_block(step, ordered_ref, field_ref, weight_ref, floors_ref, halo_ref, halo_buf):
    blocks = ordered_ref.shape[0]
    side = lax.axis_index("depth")
    halo = halo_ref[...]
    if step == 0:
        halo = jnp.dot(halo, split_matrix(halo.shape[1]).astype(BF16), preferred_element_type=F32).astype(BF16)
    b = (blocks - 1) * (1 - side)
    size = 2 * BS
    at = pl.multiple_of(b * size, size)
    halo_buf[size : 2 * size, :] = field_ref[pl.ds(at + size, size), :]
    inner = pl.multiple_of(at + 2 * size * side, size)
    halo_buf[pl.ds(pl.multiple_of(2 * size * side, size), size), :] = field_ref[pl.ds(inner, size), :]
    put_block(halo_buf, 2 * (1 - side), halo)
    first_row = side * (blocks * BS)
    field = advanced(ordered_ref[b], halo_buf[...], weight_ref[...], b * BS, floors_ref[step] - first_row)
    return b, field


def edge_step(step):
    def kernel(ordered_ref, field_ref, weight_ref, floors_ref, halo_ref, in_ref, next_ref, out_ref, halo_buf):
        del in_ref
        b, field = edge_block(step, ordered_ref, field_ref, weight_ref, floors_ref, halo_ref, halo_buf)
        out_ref[...] = field
        put_block(next_ref, b + 1, field)

    return kernel


def edge_and_pick(
    ordered_ref, field_ref, weight_ref, floors_ref, halo_ref, in_ref, receivers_ref,
    final_ref, keep_ref, send_ref, halo_buf, picked,
):
    del in_ref
    b, field = edge_block(STEPS - 1, ordered_ref, field_ref, weight_ref, floors_ref, halo_ref, halo_buf)
    final_ref[pl.ds(pl.multiple_of(b * BS, BS), BS), :] = field.astype(F32)
    rows = ordered_ref.shape[0] * BS
    side = lax.axis_index("depth")
    owned = keep_ref.shape[0]
    group = 8
    for out_ref, owner in ((send_ref, 1 - side), (keep_ref, side)):

        def some(n, carry):
            for j in range(group):
                local = receivers_ref[owner * owned + n * group + j] - side * rows
                inside = jnp.logical_and(local >= 0, local < rows)
                at = jnp.where(inside, local, rows)
                picked[pl.ds(n * group + j, 1), :] = final_ref[pl.ds(at, 1), :]
            return carry

        lax.fori_loop(0, owned // group, some, 0)
        out_ref[...] = picked[...].astype(BF16)


def basis_kernel(freq_ref, out_ref):
    core = lax.axis_index("core")
    spread = 32
    lanes = freq_ref.shape[1]
    chip = (lax.axis_index("x") * lax.axis_size("y") + lax.axis_index("y")) * lax.axis_size("zh") + lax.axis_index("zh")
    turn = 2.0 * math.pi

    def unit(count_times_freq):
        cycles = count_times_freq * (1.0 / NT)
        angle = turn * (cycles - jnp.floor(cycles))
        return jnp.cos(angle), jnp.sin(angle)

    sample = (core * spread + lax.broadcasted_iota(jnp.int32, (spread, lanes), 0)).astype(F32)
    state = []
    turns = []
    for which in (core, 1 - core):
        freq = jnp.broadcast_to(freq_ref[pl.ds(chip * 2 + which, 1), :], (spread, lanes))
        state += list(unit(freq * sample))
        turns.append(unit(freq * (2.0 * spread)))

    def some(q, state):
        at = pl.multiple_of(q * spread, spread)
        out = []
        for which in range(2):
            c, s = state[2 * which], state[2 * which + 1]
            tc, ts = turns[which]
            out_ref[pl.ds(at, spread), 2 * which * lanes : (2 * which + 1) * lanes] = c.astype(BF16)
            out_ref[pl.ds(at, spread), (2 * which + 1) * lanes : (2 * which + 2) * lanes] = (-s).astype(BF16)
            out += [c * tc - s * ts, s * tc + c * ts]
        return tuple(out)

    lax.fori_loop(0, NT // (2 * spread), some, tuple(state))


def series_kernel(basis_ref, keep_ref, got_ref, keep2_ref, got2_ref, out_ref):
    picked = jnp.concatenate([keep_ref[...] + got_ref[...], keep2_ref[...] + got2_ref[...]], axis=1)
    product = lax.dot_general(basis_ref[...], picked, (((1,), (1,)), ((), ())), preferred_element_type=F32)
    out_ref[...] = product.astype(BF16)


def local(pressure_field, block_main, block_coupled, coupling, frequencies, receivers, floors):
    rows, width = pressure_field.shape
    blocks = rows // BS
    side = lax.axis_index("depth")
    swap = [(0, 1), (1, 0)]
    halo = lax.ppermute(lax.dynamic_slice_in_dim(pressure_field, (1 - side) * (rows - BS), BS, 0), "depth", swap)

    padded = ((blocks + 2) * 2 * BS, width)
    halo_buf = pltpu.VMEM((6 * BS, width), BF16)
    ordered, start, field, weights = pl.pallas_call(
        first_step,
        out_shape=(
            vmem((blocks, 2 * BS, 6 * BS), BF16),
            vmem(padded, BF16),
            vmem(padded, BF16),
            vmem((8, width), F32),
        ),
        in_specs=[HBM_SPEC] * 5,
        out_specs=(VMEM_SPEC,) * 4,
        scratch_shapes=[
            pltpu.VMEM((rows * 6, BS), BF16),
            pltpu.VMEM((rows * 6, BS), BF16),
            pltpu.VMEM((rows, width), BF16),
            pltpu.VMEM((2 * blocks // CHUNKS, BS * 6, BS), F32),
            pltpu.VMEM((1, width), F32),
            pltpu.SMEM((STEPS,), jnp.int32),
            pltpu.SemaphoreType.DMA((3, CHUNKS)),
            pltpu.SemaphoreType.DMA((2,)),
        ],
        compiler_params=limit(28),
        name="first_step",
    )(
        in_hbm(block_main.reshape(rows * 6, BS)),
        in_hbm(block_coupled.reshape(rows * 6, BS)),
        in_hbm(pressure_field),
        in_hbm(coupling.reshape(1, width)),
        in_hbm(floors),
    )

    before = start
    for step in range(STEPS - 1):
        field, edge = pl.pallas_call(
            edge_step(step),
            out_shape=(vmem(padded, BF16), vmem((BS, width), BF16)),
            in_specs=[VMEM_SPEC] * 3 + [SMEM_SPEC] + [VMEM_SPEC] * 2,
            out_specs=(VMEM_SPEC,) * 2,
            input_output_aliases={5: 0},
            scratch_shapes=[halo_buf],
            compiler_params=limit(6),
            name="edge_step",
        )(ordered, before, weights, floors, halo, field)
        halo = lax.ppermute(edge, "depth", swap)
        last = step == STEPS - 2
        before = field
        field = pl.pallas_call(
            whole_step(step + 1, last),
            out_shape=vmem((rows + 8, width), F32) if last else vmem(padded, BF16),
            in_specs=[VMEM_SPEC] * 3 + [SMEM_SPEC],
            out_specs=VMEM_SPEC,
            compiler_params=limit(6),
            name="whole_step",
        )(ordered, before, weights, floors)

    owned = receivers.shape[0] // lax.axis_size("depth")
    _, keep, send = pl.pallas_call(
        edge_and_pick,
        out_shape=(vmem((rows + 8, width), F32), vmem((owned, width), BF16), vmem((owned, width), BF16)),
        in_specs=[VMEM_SPEC] * 3 + [SMEM_SPEC] + [VMEM_SPEC] * 2 + [SMEM_SPEC],
        out_specs=(VMEM_SPEC,) * 3,
        input_output_aliases={5: 0},
        scratch_shapes=[halo_buf, pltpu.VMEM((owned, width), F32)],
        compiler_params=limit(6),
        name="edge_and_pick",
    )(ordered, before, weights, floors, halo, field, receivers)

    got = lax.ppermute(send, "depth", swap)
    keep2 = lax.ppermute(keep, "core", swap)
    basis = pl.pallas_call(
        basis_kernel,
        out_shape=vmem((NT // 2, 2 * width), BF16),
        in_specs=[VMEM_SPEC],
        out_specs=VMEM_SPEC,
        compiler_params=limit(8),
        name="basis",
    )(frequencies.reshape(-1, width // 2))
    got2 = lax.ppermute(got, "core", swap)
    partial = pl.pallas_call(
        series_kernel,
        out_shape=jax.ShapeDtypeStruct((NT // 2, owned), BF16),
        in_specs=[VMEM_SPEC] * 5,
        out_specs=VMEM_SPEC,
        compiler_params=limit(8),
        name="series",
    )(basis, keep, got, keep2, got2)
    others = ("x", "y", "zh")
    groups = lax.axis_size(others)
    arrived = lax.all_to_all(
        partial.reshape(groups, NT // 2 // groups, owned), others, split_axis=0, concat_axis=0, tiled=True
    )
    summed = arrived.astype(F32).sum(axis=0) * (1.0 / math.sqrt(frequencies.shape[0]))
    return summed.T


def solution(mesh):
    chips = Mesh(mesh.devices.reshape(4, 4, 2, 2, 2), ("x", "y", "zh", "core", "depth"))
    freq = ("x", "y", "zh", "core")
    in_specs = (
        P("depth", freq),
        P("depth", None, None, None),
        P("depth", None, None, None),
        P(freq),
        P(),
        P(),
        P(),
    )
    return jax.shard_map(local, mesh=chips, in_specs=in_specs, out_specs=P("depth", freq), check_vma=False)
```

```python
import math

import jax
import jax.numpy as jnp
from jax import lax
from jax.experimental import pallas as pl
from jax.experimental.pallas import tpu as pltpu
from jax.sharding import Mesh, PartitionSpec as P

NT = 2048
STEPS = 4
BS = 128
F32 = jnp.float32
BF16 = jnp.bfloat16
CHUNKS = 8
AHEAD = 2
UNROLL = 8

VMEM_SPEC = pl.BlockSpec(memory_space=pltpu.VMEM)
HBM_SPEC = pl.BlockSpec(memory_space=pl.ANY)


def limit(mebibytes):
    return pltpu.CompilerParams(vmem_limit_bytes=mebibytes << 20)


def in_hbm(x):
    return pltpu.with_memory_space_constraint(x, pltpu.HBM)


def vmem(shape, dtype):
    return pltpu.VMEM(shape, dtype)


def split_matrix(width):
    half = width // 2
    source = lax.broadcasted_iota(jnp.int32, (width, width), 0)
    target = lax.broadcasted_iota(jnp.int32, (width, width), 1)
    return jnp.where(source == 2 * (target % half) + target // half, 1.0, 0.0).astype(F32)


def put_block(ref, b, field):
    half = field.shape[1] // 2
    at = b * (2 * BS)
    if not isinstance(at, int):
        at = pl.multiple_of(at, 2 * BS)
    real = field[:, :half]
    imag = field[:, half:]
    ref[0, pl.ds(at, BS), :] = real
    ref[1, pl.ds(at, BS), :] = imag
    ref[0, pl.ds(at + BS, BS), :] = -imag
    ref[1, pl.ds(at + BS, BS), :] = real


def three_blocks(ref, b):
    at = b * (2 * BS)
    if not isinstance(at, int):
        at = pl.multiple_of(at, 2 * BS)
    return jnp.concatenate([ref[0, pl.ds(at, 6 * BS), :], ref[1, pl.ds(at, 6 * BS), :]], axis=1)


def operator_rows(ordered_ref, b):
    return jnp.concatenate([ordered_ref[b, m] for m in range(ordered_ref.shape[1])], axis=1)


def advanced(ordered, stacked, weights, first_row, floor_rows):
    product = jnp.dot(ordered, stacked, preferred_element_type=F32)
    size = product.shape[0] // 2
    half = product.shape[1] // 2
    wr = weights[0:1, :half]
    wi = weights[0:1, half:]
    side_real = product[size:, :half]
    side_imag = product[size:, half:]
    real = product[:size, :half] + (wr * side_real - wi * side_imag)
    imag = product[:size, half:] + (wr * side_imag + wi * side_real)
    row = first_row + lax.broadcasted_iota(jnp.int32, (size, half), 0)
    damping = jnp.where(row >= floor_rows, 0.5, 1.0).astype(F32)
    return jnp.concatenate([damping * real, damping * imag], axis=1).astype(BF16)


def put_final(ref, at, field):
    half = field.shape[1] // 2
    ref[0, pl.ds(at, BS), :] = field[:, :half].astype(F32)
    ref[1, pl.ds(at, BS), :] = field[:, half:].astype(F32)


def zero_ends(ref):
    edge = jnp.zeros((2, 2 * BS, ref.shape[2]), ref.dtype)
    ref[:, 0 : 2 * BS, :] = edge
    ref[:, ref.shape[1] - 2 * BS :, :] = edge


def first_step(
    main_hbm, side_hbm, field_hbm, coupling_hbm, floors_hbm,
    receivers_hbm, ordered_ref, start_ref, next_ref, weight_ref, floor_ref, pick_ref,
    main_buf, side_buf, field_buf, planes, coupling_buf, floors_buf, receivers_buf, sems, small_sems,
):
    blocks = ordered_ref.shape[0]
    per = blocks // CHUNKS
    rows = per * BS
    op_rows = rows * 6
    width = field_buf.shape[1]
    coupling_copy = pltpu.make_async_copy(coupling_hbm, coupling_buf, small_sems.at[0])
    floors_copy = pltpu.make_async_copy(floors_hbm, floors_buf, small_sems.at[1])
    receivers_copy = pltpu.make_async_copy(receivers_hbm, receivers_buf, small_sems.at[2])
    coupling_copy.start()
    floors_copy.start()
    receivers_copy.start()
    copies = []
    for n in range(CHUNKS):
        copies.append(
            [
                pltpu.make_async_copy(
                    source.at[pl.ds(n * size, size), :], buf.at[pl.ds(n * size, size), :], sems.at[kind, n]
                )
                for kind, (source, buf, size) in enumerate(
                    ((field_hbm, field_buf, rows), (main_hbm, main_buf, op_rows), (side_hbm, side_buf, op_rows))
                )
            ]
        )
    copies[0][0].start()
    for n in range(AHEAD):
        copies[n + 1][0].start()
        copies[n][1].start()
        copies[n][2].start()
    perm = split_matrix(width)
    for ref in (start_ref, next_ref):
        zero_ends(ref)
    coupling_copy.wait()
    floors_copy.wait()
    weights = jnp.dot(
        jnp.broadcast_to(coupling_buf[...], (8, width)), perm, preferred_element_type=F32, precision=lax.Precision.HIGHEST
    )
    weight_ref[...] = weights
    perm = perm.astype(BF16)
    first_row = lax.axis_index("depth") * (blocks * BS)
    lanes = floor_ref.shape
    floors = jnp.zeros(lanes, jnp.int32)
    for step in range(STEPS):
        floors = jnp.where(lax.broadcasted_iota(jnp.int32, lanes, 0) == step, floors_buf[step] - first_row, floors)
    floor_ref[...] = floors
    receivers_copy.wait()
    local = receivers_buf[...] - first_row
    pick_ref[...] = jnp.where(jnp.logical_and(local >= 0, local < blocks * BS), local, blocks * BS)

    def split_chunk(n):
        for j in range(per):
            b = n * per + j
            field = jnp.dot(field_buf[b * BS : (b + 1) * BS, :], perm, preferred_element_type=F32).astype(BF16)
            put_block(start_ref, b + 1, field)

    def order_block(n, j):
        b = n * per + j
        for kind, buf in enumerate((main_buf, side_buf)):
            plane = planes.at[(n % 2) * 2 * per + j * 2 + kind]
            plane[...] = buf[b * BS * 6 : (b + 1) * BS * 6, :].astype(F32)
            for m in range(6):
                ordered_ref[b, m, kind * BS : (kind + 1) * BS, :] = plane[pl.ds(m, BS, stride=6), :].astype(BF16)

    def march_block(b):
        field = advanced(
            operator_rows(ordered_ref, b), three_blocks(start_ref, b), weights, b * BS, floors[0:1, : width // 2]
        )
        put_block(next_ref, b + 1, field)

    always = lax.axis_index("depth") >= 0
    copies[0][0].wait()
    split_chunk(0)
    for n in range(CHUNKS + 1):
        if n < CHUNKS:
            copies[n][1].wait()
            copies[n][2].wait()
            if n + AHEAD < CHUNKS:
                copies[n + AHEAD][1].start()
                copies[n + AHEAD][2].start()
                if n + AHEAD + 1 < CHUNKS:
                    copies[n + AHEAD + 1][0].start()
            if n + 1 < CHUNKS:
                copies[n + 1][0].wait()

        @pl.when(always)
        def _(n=n):
            for j in range(per):
                if n > 0:
                    march_block((n - 1) * per + j)
                if n < CHUNKS:
                    order_block(n, j)
            if n + 1 < CHUNKS:
                split_chunk(n + 1)


def whole_step(step, last):
    def kernel(ordered_ref, field_ref, weight_ref, floor_ref, next_ref):
        blocks = ordered_ref.shape[0]
        floors = floor_ref[step : step + 1, :]
        weights = weight_ref[...]
        if last:
            next_ref[:, blocks * BS :, :] = jnp.zeros((2, next_ref.shape[1] - blocks * BS, next_ref.shape[2]), F32)
        else:
            zero_ends(next_ref)

        def some(n, carry):
            for j in range(UNROLL):
                b = n * UNROLL + j
                at = pl.multiple_of(b * BS, BS)
                field = advanced(operator_rows(ordered_ref, b), three_blocks(field_ref, b), weights, at, floors)
                if last:
                    put_final(next_ref, at, field)
                else:
                    put_block(next_ref, b + 1, field)
            return carry

        lax.fori_loop(0, blocks // UNROLL, some, 0)

    return kernel


def edge_block(step, ordered_ref, field_ref, weight_ref, floor_ref, halo_ref, halo_buf):
    blocks = ordered_ref.shape[0]
    side = lax.axis_index("depth")
    halo = halo_ref[...]
    if step == 0:
        halo = jnp.dot(halo, split_matrix(halo.shape[1]).astype(BF16), preferred_element_type=F32).astype(BF16)
    b = (blocks - 1) * (1 - side)
    size = 2 * BS
    at = pl.multiple_of(b * size, size)
    halo_buf[:, size : 2 * size, :] = field_ref[:, pl.ds(at + size, size), :]
    inner = pl.multiple_of(at + 2 * size * side, size)
    halo_buf[:, pl.ds(pl.multiple_of(2 * size * side, size), size), :] = field_ref[:, pl.ds(inner, size), :]
    put_block(halo_buf, 2 * (1 - side), halo)
    field = advanced(
        operator_rows(ordered_ref, b), three_blocks(halo_buf, 0), weight_ref[...], b * BS, floor_ref[step : step + 1, :]
    )
    return b, field


def edge_step(step):
    def kernel(ordered_ref, field_ref, weight_ref, floor_ref, halo_ref, in_ref, next_ref, out_ref, halo_buf):
        del in_ref
        b, field = edge_block(step, ordered_ref, field_ref, weight_ref, floor_ref, halo_ref, halo_buf)
        out_ref[...] = field
        put_block(next_ref, b + 1, field)

    return kernel


def edge_and_pick(
    ordered_ref, field_ref, weight_ref, floor_ref, halo_ref, in_ref, rows_vmem,
    final_ref, keep_ref, send_ref, halo_buf, picked, rows_ref, sem,
):
    del in_ref
    rows_copy = pltpu.make_async_copy(rows_vmem, rows_ref, sem)
    rows_copy.start()
    b, field = edge_block(STEPS - 1, ordered_ref, field_ref, weight_ref, floor_ref, halo_ref, halo_buf)
    put_final(final_ref, pl.multiple_of(b * BS, BS), field)
    side = lax.axis_index("depth")
    owned = keep_ref.shape[0]
    lanes = rows_ref.shape[1]
    group = 32
    rows_copy.wait()
    for out_ref, owner in ((send_ref, 1 - side), (keep_ref, side)):

        def some(n, carry):
            for j in range(group):
                at = rows_ref[owner * (owned // lanes) + n // (lanes // group), (n % (lanes // group)) * group + j]
                picked[0, pl.ds(n * group + j, 1), :] = final_ref[0, pl.ds(at, 1), :]
                picked[1, pl.ds(n * group + j, 1), :] = final_ref[1, pl.ds(at, 1), :]
            return carry

        lax.fori_loop(0, owned // group, some, 0)
        out_ref[...] = jnp.concatenate([picked[0], picked[1]], axis=1).astype(BF16)


def basis_kernel(freq_ref, out_ref):
    core = lax.axis_index("core")
    spread = 32
    lanes = freq_ref.shape[1]
    chip = (lax.axis_index("x") * lax.axis_size("y") + lax.axis_index("y")) * lax.axis_size("zh") + lax.axis_index("zh")
    turn = 2.0 * math.pi

    def unit(count_times_freq):
        cycles = count_times_freq * (1.0 / NT)
        angle = turn * (cycles - jnp.floor(cycles))
        return jnp.cos(angle), jnp.sin(angle)

    sample = (core * spread + lax.broadcasted_iota(jnp.int32, (spread, lanes), 0)).astype(F32)
    state = []
    turns = []
    for which in (core, 1 - core):
        freq = jnp.broadcast_to(freq_ref[pl.ds(chip * 2 + which, 1), :], (spread, lanes))
        state += list(unit(freq * sample))
        turns.append(unit(freq * (2.0 * spread)))

    def some(q, state):
        at = pl.multiple_of(q * spread, spread)
        out = []
        for which in range(2):
            c, s = state[2 * which], state[2 * which + 1]
            tc, ts = turns[which]
            out_ref[pl.ds(at, spread), 2 * which * lanes : (2 * which + 1) * lanes] = c.astype(BF16)
            out_ref[pl.ds(at, spread), (2 * which + 1) * lanes : (2 * which + 2) * lanes] = (-s).astype(BF16)
            out += [c * tc - s * ts, s * tc + c * ts]
        return tuple(out)

    lax.fori_loop(0, NT // (2 * spread), some, tuple(state))


def series_kernel(basis_ref, keep_ref, got_ref, keep2_ref, got2_ref, out_ref):
    picked = jnp.concatenate([keep_ref[...] + got_ref[...], keep2_ref[...] + got2_ref[...]], axis=1)
    product = lax.dot_general(basis_ref[...], picked, (((1,), (1,)), ((), ())), preferred_element_type=F32)
    out_ref[...] = product.astype(BF16)


def local(pressure_field, block_main, block_coupled, coupling, frequencies, receivers, floors):
    rows, width = pressure_field.shape
    blocks = rows // BS
    side = lax.axis_index("depth")
    swap = [(0, 1), (1, 0)]
    halo = lax.ppermute(lax.dynamic_slice_in_dim(pressure_field, (1 - side) * (rows - BS), BS, 0), "depth", swap)

    padded = (2, (blocks + 2) * 2 * BS, width // 2)
    halo_buf = pltpu.VMEM((2, 6 * BS, width // 2), BF16)
    ordered, start, field, weights, floor_rows, pick_rows = pl.pallas_call(
        first_step,
        out_shape=(
            vmem((blocks, 6, 2 * BS, BS), BF16),
            vmem(padded, BF16),
            vmem(padded, BF16),
            vmem((8, width), F32),
            vmem((8, width // 2), jnp.int32),
            vmem((receivers.shape[0] // BS, BS), jnp.int32),
        ),
        in_specs=[HBM_SPEC] * 6,
        out_specs=(VMEM_SPEC,) * 6,
        scratch_shapes=[
            pltpu.VMEM((rows * 6, BS), BF16),
            pltpu.VMEM((rows * 6, BS), BF16),
            pltpu.VMEM((rows, width), BF16),
            pltpu.VMEM((4 * blocks // CHUNKS, BS * 6, BS), F32),
            pltpu.VMEM((1, width), F32),
            pltpu.SMEM((STEPS,), jnp.int32),
            pltpu.VMEM((receivers.shape[0] // BS, BS), jnp.int32),
            pltpu.SemaphoreType.DMA((3, CHUNKS)),
            pltpu.SemaphoreType.DMA((3,)),
        ],
        compiler_params=limit(28),
        name="first_step",
    )(
        in_hbm(block_main.reshape(rows * 6, BS)),
        in_hbm(block_coupled.reshape(rows * 6, BS)),
        in_hbm(pressure_field),
        in_hbm(coupling.reshape(1, width)),
        in_hbm(floors),
        in_hbm(receivers.reshape(-1, BS)),
    )

    before = start
    for step in range(STEPS - 1):
        field, edge = pl.pallas_call(
            edge_step(step),
            out_shape=(vmem(padded, BF16), vmem((BS, width), BF16)),
            in_specs=[VMEM_SPEC] * 6,
            out_specs=(VMEM_SPEC,) * 2,
            input_output_aliases={5: 0},
            scratch_shapes=[halo_buf],
            compiler_params=limit(6),
            name="edge_step",
        )(ordered, before, weights, floor_rows, halo, field)
        halo = lax.ppermute(edge, "depth", swap)
        last = step == STEPS - 2
        before = field
        field = pl.pallas_call(
            whole_step(step + 1, last),
            out_shape=vmem((2, rows + 8, width // 2), F32) if last else vmem(padded, BF16),
            in_specs=[VMEM_SPEC] * 4,
            out_specs=VMEM_SPEC,
            compiler_params=limit(6),
            name="whole_step",
        )(ordered, before, weights, floor_rows)

    owned = receivers.shape[0] // lax.axis_size("depth")
    _, keep, send = pl.pallas_call(
        edge_and_pick,
        out_shape=(vmem((2, rows + 8, width // 2), F32), vmem((owned, width), BF16), vmem((owned, width), BF16)),
        in_specs=[VMEM_SPEC] * 7,
        out_specs=(VMEM_SPEC,) * 3,
        input_output_aliases={5: 0},
        scratch_shapes=[
            halo_buf,
            pltpu.VMEM((2, owned, width // 2), F32),
            pltpu.SMEM(pick_rows.shape, jnp.int32),
            pltpu.SemaphoreType.DMA,
        ],
        compiler_params=limit(6),
        name="edge_and_pick",
    )(ordered, before, weights, floor_rows, halo, field, pick_rows)

    got = lax.ppermute(send, "depth", swap)
    keep2 = lax.ppermute(keep, "core", swap)
    basis = pl.pallas_call(
        basis_kernel,
        out_shape=vmem((NT // 2, 2 * width), BF16),
        in_specs=[VMEM_SPEC],
        out_specs=VMEM_SPEC,
        compiler_params=limit(8),
        cost_estimate=pl.CostEstimate(flops=4_000_000_000, bytes_accessed=0, transcendentals=0),
        name="basis",
    )(frequencies.reshape(-1, width // 2))
    got2 = lax.ppermute(got, "core", swap)
    partial = pl.pallas_call(
        series_kernel,
        out_shape=jax.ShapeDtypeStruct((NT // 2, owned), BF16),
        in_specs=[VMEM_SPEC] * 5,
        out_specs=VMEM_SPEC,
        compiler_params=limit(8),
        name="series",
    )(basis, keep, got, keep2, got2)
    others = ("x", "y", "zh")
    groups = lax.axis_size(others)
    arrived = lax.all_to_all(
        partial.reshape(groups, NT // 2 // groups, owned), others, split_axis=0, concat_axis=0, tiled=True
    )
    summed = arrived.astype(F32).sum(axis=0) * (1.0 / math.sqrt(frequencies.shape[0]))
    return summed.T


def solution(mesh):
    chips = Mesh(mesh.devices.reshape(4, 4, 2, 2, 2), ("x", "y", "zh", "core", "depth"))
    freq = ("x", "y", "zh", "core")
    in_specs = (
        P("depth", freq),
        P("depth", None, None, None),
        P("depth", None, None, None),
        P(freq),
        P(),
        P(),
        P(),
    )
    return jax.shard_map(local, mesh=chips, in_specs=in_specs, out_specs=P("depth", freq), check_vma=False)
```

```python
import math

import jax
import jax.numpy as jnp
from jax import lax
from jax.experimental import pallas as pl
from jax.experimental.pallas import tpu as pltpu
from jax.sharding import Mesh, PartitionSpec as P


NT = 2048
STEPS = 4
BS = 128
F32 = jnp.float32
BF16 = jnp.bfloat16
CHUNKS = 8
AHEAD = 3
UNROLL = 32

VMEM_SPEC = pl.BlockSpec(memory_space=pltpu.VMEM)
HBM_SPEC = pl.BlockSpec(memory_space=pl.ANY)


def limit(mebibytes):
    return pltpu.CompilerParams(vmem_limit_bytes=mebibytes << 20)


def in_hbm(x):
    return pltpu.with_memory_space_constraint(x, pltpu.HBM)


def vmem(shape, dtype):
    return pltpu.VMEM(shape, dtype)


def split_matrix(width):
    half = width // 2
    source = lax.broadcasted_iota(jnp.int32, (width, width), 0)
    target = lax.broadcasted_iota(jnp.int32, (width, width), 1)
    return jnp.where(source == 2 * (target % half) + target // half, 1.0, 0.0).astype(F32)


def put_block(ref, b, field):
    half = field.shape[1] // 2
    at = b * (2 * BS)
    if not isinstance(at, int):
        at = pl.multiple_of(at, 2 * BS)
    real = field[:, :half]
    imag = field[:, half:]
    ref[0, pl.ds(at, BS), :] = real
    ref[1, pl.ds(at, BS), :] = imag
    ref[0, pl.ds(at + BS, BS), :] = -imag
    ref[1, pl.ds(at + BS, BS), :] = real


def three_blocks(ref, b):
    at = b * (2 * BS)
    if not isinstance(at, int):
        at = pl.multiple_of(at, 2 * BS)
    return jnp.concatenate([ref[0, pl.ds(at, 6 * BS), :], ref[1, pl.ds(at, 6 * BS), :]], axis=1)


def operator_rows(ordered_ref, b):
    return jnp.concatenate([ordered_ref[b, m] for m in range(ordered_ref.shape[1])], axis=1)


def advanced(ordered, stacked, weights, first_row, floor_rows):
    product = jnp.dot(ordered, stacked, preferred_element_type=F32)
    size = product.shape[0] // 2
    half = product.shape[1] // 2
    wr = weights[0:1, :half]
    wi = weights[0:1, half:]
    side_real = product[size:, :half]
    side_imag = product[size:, half:]
    real = product[:size, :half] + (wr * side_real - wi * side_imag)
    imag = product[:size, half:] + (wr * side_imag + wi * side_real)
    row = first_row + lax.broadcasted_iota(jnp.int32, (size, half), 0)
    damping = jnp.where(row >= floor_rows, 0.5, 1.0).astype(F32)
    return jnp.concatenate([damping * real, damping * imag], axis=1).astype(BF16)


def put_final(ref, at, field):
    half = field.shape[1] // 2
    ref[0, pl.ds(at, BS), :] = field[:, :half].astype(F32)
    ref[1, pl.ds(at, BS), :] = field[:, half:].astype(F32)


def zero_ends(ref):
    edge = jnp.zeros((2, 2 * BS, ref.shape[2]), ref.dtype)
    ref[:, 0 : 2 * BS, :] = edge
    ref[:, ref.shape[1] - 2 * BS :, :] = edge


def load(
    main_hbm, side_hbm, field_hbm, coupling_hbm, floors_hbm,
    receivers_hbm, ordered_ref, start_ref, edge_ref, weight_ref, floor_ref, pick_ref,
    main_buf, side_buf, field_buf, planes, perm_ref, coupling_buf, floors_buf, receivers_buf, sems, small_sems,
):
    blocks = ordered_ref.shape[0]
    per = blocks // CHUNKS
    rows = per * BS
    op_rows = rows * 6
    width = field_buf.shape[1]
    coupling_copy = pltpu.make_async_copy(coupling_hbm, coupling_buf, small_sems.at[0])
    floors_copy = pltpu.make_async_copy(floors_hbm, floors_buf, small_sems.at[1])
    receivers_copy = pltpu.make_async_copy(receivers_hbm, receivers_buf, small_sems.at[2])
    coupling_copy.start()
    floors_copy.start()
    receivers_copy.start()
    copies = []
    for n in range(CHUNKS):
        copies.append(
            [
                pltpu.make_async_copy(
                    source.at[pl.ds(n * size, size), :], buf.at[pl.ds(n * size, size), :], sems.at[kind, n]
                )
                for kind, (source, buf, size) in enumerate(
                    ((field_hbm, field_buf, rows), (main_hbm, main_buf, op_rows), (side_hbm, side_buf, op_rows))
                )
            ]
        )
    for n in range(AHEAD):
        for kind in range(3):
            copies[n][kind].start()
    perm_ref[...] = split_matrix(width).astype(BF16)
    first_row = lax.axis_index("depth") * (blocks * BS)

    def small_tables():
        zero_ends(start_ref)
        weight_ref[...] = jnp.dot(
            jnp.broadcast_to(coupling_buf[...], (8, width)),
            split_matrix(width),
            preferred_element_type=F32,
            precision=lax.Precision.HIGHEST,
        )
        shape = floor_ref.shape
        floors = jnp.zeros(shape, jnp.int32)
        for step in range(STEPS):
            floors = jnp.where(lax.broadcasted_iota(jnp.int32, shape, 0) == step, floors_buf[step] - first_row, floors)
        floor_ref[...] = floors
        local = receivers_buf[...] - first_row
        local = jnp.where(jnp.logical_and(local >= 0, local < blocks * BS), local, blocks * BS)
        mine = local.shape[0] // 2
        turned = jnp.concatenate([local[mine:], local[:mine]], axis=0)
        pick_ref[...] = jnp.where(lax.axis_index("depth") == 0, turned, local)

    def split_chunk(n):
        for j in range(per):
            b = n * per + j
            field = jnp.dot(field_buf[b * BS : (b + 1) * BS, :], perm_ref[...], preferred_element_type=F32).astype(BF16)
            put_block(start_ref, b + 1, field)

    def order_block(n, j, kind):
        b = n * per + j
        buf = (main_buf, side_buf)[kind]
        plane = planes.at[(n % 2) * 2 * per + j * 2 + kind]
        plane[...] = buf[b * BS * 6 : (b + 1) * BS * 6, :].astype(F32)
        for m in range(6):
            ordered_ref[b, m, kind * BS : (kind + 1) * BS, :] = plane[pl.ds(m, BS, stride=6), :].astype(BF16)

    for n in range(CHUNKS):
        for kind in range(3):
            copies[n][kind].wait()
            if n + AHEAD < CHUNKS:
                copies[n + AHEAD][kind].start()
        split_chunk(n)
        for j in range(per):
            order_block(n, j, 0)
            order_block(n, j, 1)
        if n == 1:
            coupling_copy.wait()
            floors_copy.wait()
            receivers_copy.wait()
            small_tables()
    edge_at = pl.multiple_of((1 + (blocks - 1) * (1 - lax.axis_index("depth"))) * 2 * BS, 2 * BS)
    edge_ref[...] = jnp.concatenate([start_ref[0, pl.ds(edge_at, BS), :], start_ref[1, pl.ds(edge_at, BS), :]], axis=1)


def whole_step(step, last):
    def kernel(ordered_ref, field_ref, weight_ref, floor_ref, next_ref):
        blocks = ordered_ref.shape[0]
        floors = floor_ref[step : step + 1, :]
        weights = weight_ref[...]
        if last:
            next_ref[:, blocks * BS :, :] = jnp.zeros((2, next_ref.shape[1] - blocks * BS, next_ref.shape[2]), F32)
        else:
            zero_ends(next_ref)

        def some(n, carry):
            for j in range(UNROLL):
                b = n * UNROLL + j
                at = pl.multiple_of(b * BS, BS)
                field = advanced(operator_rows(ordered_ref, b), three_blocks(field_ref, b), weights, at, floors)
                if last:
                    put_final(next_ref, at, field)
                else:
                    put_block(next_ref, b + 1, field)
            return carry

        lax.fori_loop(0, blocks // UNROLL, some, 0)

    return kernel


def edge_block(step, ordered_ref, field_ref, weight_ref, floor_ref, halo_ref, halo_buf):
    blocks = ordered_ref.shape[0]
    side = lax.axis_index("depth")
    halo = halo_ref[...]
    b = (blocks - 1) * (1 - side)
    size = 2 * BS
    at = pl.multiple_of(b * size, size)
    halo_buf[:, size : 2 * size, :] = field_ref[:, pl.ds(at + size, size), :]
    inner = pl.multiple_of(at + 2 * size * side, size)
    halo_buf[:, pl.ds(pl.multiple_of(2 * size * side, size), size), :] = field_ref[:, pl.ds(inner, size), :]
    put_block(halo_buf, 2 * (1 - side), halo)
    field = advanced(
        operator_rows(ordered_ref, b), three_blocks(halo_buf, 0), weight_ref[...], b * BS, floor_ref[step : step + 1, :]
    )
    return b, field


def edge_step(step):
    def kernel(ordered_ref, field_ref, weight_ref, floor_ref, halo_ref, in_ref, next_ref, out_ref, halo_buf):
        del in_ref
        b, field = edge_block(step, ordered_ref, field_ref, weight_ref, floor_ref, halo_ref, halo_buf)
        out_ref[...] = field
        put_block(next_ref, b + 1, field)

    return kernel


def edge_and_pick(
    ordered_ref, field_ref, weight_ref, floor_ref, halo_ref, in_ref, rows_vmem,
    final_ref, keep_ref, send_ref, halo_buf, picked, rows_ref, sem,
):
    del in_ref
    rows_copy = pltpu.make_async_copy(rows_vmem, rows_ref, sem)
    rows_copy.start()
    b, field = edge_block(STEPS - 1, ordered_ref, field_ref, weight_ref, floor_ref, halo_ref, halo_buf)
    put_final(final_ref, pl.multiple_of(b * BS, BS), field)
    owned = keep_ref.shape[0]
    lanes = rows_ref.shape[1]
    rows_copy.wait()
    for which, out_ref in enumerate((send_ref, keep_ref)):
        for n in range(owned):
            at = rows_ref[(which * owned + n) // lanes, n % lanes]
            for part in range(2):
                picked[part, n : n + 1, :] = final_ref[part, pl.ds(at, 1), :]
        out_ref[...] = jnp.concatenate([picked[0], picked[1]], axis=1).astype(BF16)


def basis_kernel(freq_ref, out_ref):
    core = lax.axis_index("core")
    spread = 32
    lanes = freq_ref.shape[1]
    chip = (lax.axis_index("x") * lax.axis_size("y") + lax.axis_index("y")) * lax.axis_size("zh") + lax.axis_index("zh")
    turn = 2.0 * math.pi

    def unit(count_times_freq):
        cycles = count_times_freq * (1.0 / NT)
        angle = turn * (cycles - jnp.floor(cycles))
        return jnp.cos(angle), jnp.sin(angle)

    sample = (core * spread + lax.broadcasted_iota(jnp.int32, (spread, lanes), 0)).astype(F32)
    state = []
    turns = []
    for which in (core, 1 - core):
        freq = jnp.broadcast_to(freq_ref[pl.ds(chip * 2 + which, 1), :], (spread, lanes))
        state += list(unit(freq * sample))
        turns.append(unit(freq * (2.0 * spread)))

    def some(q, state):
        at = pl.multiple_of(q * spread, spread)
        out = []
        for which in range(2):
            c, s = state[2 * which], state[2 * which + 1]
            tc, ts = turns[which]
            out_ref[pl.ds(at, spread), 2 * which * lanes : (2 * which + 1) * lanes] = c.astype(BF16)
            out_ref[pl.ds(at, spread), (2 * which + 1) * lanes : (2 * which + 2) * lanes] = (-s).astype(BF16)
            out += [c * tc - s * ts, s * tc + c * ts]
        return tuple(out)

    lax.fori_loop(0, NT // (2 * spread), some, tuple(state))


def series_kernel(basis_ref, keep_ref, got_ref, keep2_ref, got2_ref, out_ref):
    picked = jnp.concatenate([keep_ref[...] + got_ref[...], keep2_ref[...] + got2_ref[...]], axis=1)
    product = lax.dot_general(basis_ref[...], picked, (((1,), (1,)), ((), ())), preferred_element_type=F32)
    out_ref[...] = product.astype(BF16)


def local(pressure_field, block_main, block_coupled, coupling, frequencies, receivers, floors):
    rows, width = pressure_field.shape
    blocks = rows // BS
    swap = [(0, 1), (1, 0)]
    padded = (2, (blocks + 2) * 2 * BS, width // 2)
    halo_buf = pltpu.VMEM((2, 6 * BS, width // 2), BF16)
    ordered, start, edge, weights, floor_rows, pick_rows = pl.pallas_call(
        load,
        out_shape=(
            vmem((blocks, 6, 2 * BS, BS), BF16),
            vmem(padded, BF16),
            vmem((BS, width), BF16),
            vmem((8, width), F32),
            vmem((8, width // 2), jnp.int32),
            vmem((receivers.shape[0] // BS, BS), jnp.int32),
        ),
        in_specs=[HBM_SPEC] * 6,
        out_specs=(VMEM_SPEC,) * 6,
        scratch_shapes=[
            pltpu.VMEM((rows * 6, BS), BF16),
            pltpu.VMEM((rows * 6, BS), BF16),
            pltpu.VMEM((rows, width), BF16),
            pltpu.VMEM((4 * blocks // CHUNKS, BS * 6, BS), F32),
            pltpu.VMEM((width, width), BF16),
            pltpu.VMEM((1, width), F32),
            pltpu.SMEM((STEPS,), jnp.int32),
            pltpu.VMEM((receivers.shape[0] // BS, BS), jnp.int32),
            pltpu.SemaphoreType.DMA((3, CHUNKS)),
            pltpu.SemaphoreType.DMA((3,)),
        ],
        compiler_params=limit(28),
        name="load",
    )(
        in_hbm(block_main.reshape(rows * 6, BS)),
        in_hbm(block_coupled.reshape(rows * 6, BS)),
        in_hbm(pressure_field),
        in_hbm(coupling.reshape(1, width)),
        in_hbm(floors),
        in_hbm(receivers.reshape(-1, BS)),
    )

    before = start
    for step in range(STEPS):
        last = step == STEPS - 1
        halo = lax.ppermute(edge, "depth", swap)
        field = pl.pallas_call(
            whole_step(step, last),
            out_shape=vmem((2, rows + 8, width // 2), F32) if last else vmem(padded, BF16),
            in_specs=[VMEM_SPEC] * 4,
            out_specs=VMEM_SPEC,
            compiler_params=limit(6),
            name="whole_step",
        )(ordered, before, weights, floor_rows)
        if last:
            break
        before, edge = pl.pallas_call(
            edge_step(step),
            out_shape=(vmem(padded, BF16), vmem((BS, width), BF16)),
            in_specs=[VMEM_SPEC] * 6,
            out_specs=(VMEM_SPEC,) * 2,
            input_output_aliases={5: 0},
            scratch_shapes=[halo_buf],
            compiler_params=limit(6),
            name="edge_step",
        )(ordered, before, weights, floor_rows, halo, field)

    owned = receivers.shape[0] // lax.axis_size("depth")
    _, keep, send = pl.pallas_call(
        edge_and_pick,
        out_shape=(vmem((2, rows + 8, width // 2), F32), vmem((owned, width), BF16), vmem((owned, width), BF16)),
        in_specs=[VMEM_SPEC] * 7,
        out_specs=(VMEM_SPEC,) * 3,
        input_output_aliases={5: 0},
        scratch_shapes=[
            halo_buf,
            pltpu.VMEM((2, owned, width // 2), F32),
            pltpu.SMEM(pick_rows.shape, jnp.int32),
            pltpu.SemaphoreType.DMA,
        ],
        compiler_params=limit(6),
        name="edge_and_pick",
    )(ordered, before, weights, floor_rows, halo, field, pick_rows)

    got = lax.ppermute(send, "depth", swap)
    keep2 = lax.ppermute(keep, "core", swap)
    basis = pl.pallas_call(
        basis_kernel,
        out_shape=vmem((NT // 2, 2 * width), BF16),
        in_specs=[VMEM_SPEC],
        out_specs=VMEM_SPEC,
        compiler_params=limit(8),
        name="basis",
    )(frequencies.reshape(-1, width // 2))
    got2 = lax.ppermute(got, "core", swap)
    partial = pl.pallas_call(
        series_kernel,
        out_shape=jax.ShapeDtypeStruct((NT // 2, owned), BF16),
        in_specs=[VMEM_SPEC] * 5,
        out_specs=VMEM_SPEC,
        compiler_params=limit(8),
        name="series",
    )(basis, keep, got, keep2, got2)
    others = ("x", "y", "zh")
    groups = lax.axis_size(others)
    arrived = lax.all_to_all(
        partial.reshape(groups, NT // 2 // groups, owned), others, split_axis=0, concat_axis=0, tiled=True
    )
    summed = arrived.astype(F32).sum(axis=0) * (1.0 / math.sqrt(frequencies.shape[0]))
    return summed.T


def solution(mesh):
    chips = Mesh(mesh.devices.reshape(4, 4, 2, 2, 2), ("x", "y", "zh", "core", "depth"))
    freq = ("x", "y", "zh", "core")
    in_specs = (
        P("depth", freq),
        P("depth", None, None, None),
        P("depth", None, None, None),
        P(freq),
        P(),
        P(),
        P(),
    )

    return jax.shard_map(local, mesh=chips, in_specs=in_specs, out_specs=P("depth", freq), check_vma=False)
```

```python
import math

import jax
import jax.numpy as jnp
from jax import lax
from jax.experimental import pallas as pl
from jax.experimental.pallas import tpu as pltpu
from jax.sharding import Mesh, PartitionSpec as P


NT = 2048
STEPS = 4
BS = 128
F32 = jnp.float32
BF16 = jnp.bfloat16
CHUNKS = (1, 3, 4, 4, 4, 4, 4, 4, 2, 2)
AHEAD = 3

VMEM_SPEC = pl.BlockSpec(memory_space=pltpu.VMEM)
HBM_SPEC = pl.BlockSpec(memory_space=pl.ANY)


def limit(mebibytes):
    return pltpu.CompilerParams(vmem_limit_bytes=mebibytes << 20)


def in_hbm(x):
    return pltpu.with_memory_space_constraint(x, pltpu.HBM)


def vmem(shape, dtype):
    return pltpu.VMEM(shape, dtype)


def split_matrix(width):
    half = width // 2
    source = lax.broadcasted_iota(jnp.int32, (width, width), 0)
    target = lax.broadcasted_iota(jnp.int32, (width, width), 1)
    return jnp.where(source == 2 * (target % half) + target // half, 1.0, 0.0).astype(F32)


def put_block(ref, b, field):
    half = field.shape[1] // 2
    at = b * (2 * BS)
    if not isinstance(at, int):
        at = pl.multiple_of(at, 2 * BS)
    real = field[:, :half]
    imag = field[:, half:]
    ref[0, pl.ds(at, BS), :] = real
    ref[1, pl.ds(at, BS), :] = imag
    ref[0, pl.ds(at + BS, BS), :] = -imag
    ref[1, pl.ds(at + BS, BS), :] = real


def three_blocks(ref, b):
    at = b * (2 * BS)
    if not isinstance(at, int):
        at = pl.multiple_of(at, 2 * BS)
    return jnp.concatenate([ref[0, pl.ds(at, 6 * BS), :], ref[1, pl.ds(at, 6 * BS), :]], axis=1)


def operator_rows(ordered_ref, b):
    return jnp.concatenate([ordered_ref[b, m] for m in range(ordered_ref.shape[1])], axis=1)


def advanced(ordered, stacked, weights, first_row, floor_rows):
    return finished(jnp.dot(ordered, stacked, preferred_element_type=F32), weights, first_row, floor_rows)


def finished(product, weights, first_row, floor_rows):
    size = product.shape[0] // 2
    half = product.shape[1] // 2
    wr = weights[0:1, :half]
    wi = weights[0:1, half:]
    side_real = product[size:, :half]
    side_imag = product[size:, half:]
    real = product[:size, :half] + (wr * side_real - wi * side_imag)
    imag = product[:size, half:] + (wr * side_imag + wi * side_real)
    row = first_row + lax.broadcasted_iota(jnp.int32, (size, half), 0)
    damping = jnp.where(row >= floor_rows, 0.5, 1.0).astype(F32)
    return jnp.concatenate([damping * real, damping * imag], axis=1).astype(BF16)


def put_final(ref, at, field):
    half = field.shape[1] // 2
    ref[0, pl.ds(at, BS), :] = field[:, :half].astype(F32)
    ref[1, pl.ds(at, BS), :] = field[:, half:].astype(F32)


def zero_ends(ref):
    edge = jnp.zeros((2, 2 * BS, ref.shape[2]), ref.dtype)
    ref[:, 0 : 2 * BS, :] = edge
    ref[:, ref.shape[1] - 2 * BS :, :] = edge


def chunk_sizes(blocks):
    return [part * blocks // sum(CHUNKS) for part in CHUNKS]


def load(
    main_hbm, side_hbm, field_hbm, coupling_hbm, floors_hbm,
    receivers_hbm, ordered_ref, start_ref, edge_ref, weight_ref, floor_ref, pick_ref,
    main_buf, side_buf, field_buf, planes, perm_ref, coupling_buf, floors_buf, receivers_buf, sems, small_sems,
):
    blocks = ordered_ref.shape[0]
    sizes = chunk_sizes(blocks)
    firsts = [sum(sizes[:n]) for n in range(len(sizes))]
    width = field_buf.shape[1]
    coupling_copy = pltpu.make_async_copy(coupling_hbm, coupling_buf, small_sems.at[0])
    floors_copy = pltpu.make_async_copy(floors_hbm, floors_buf, small_sems.at[1])
    receivers_copy = pltpu.make_async_copy(receivers_hbm, receivers_buf, small_sems.at[2])
    coupling_copy.start()
    floors_copy.start()
    receivers_copy.start()
    copies = []
    for n, (first, count) in enumerate(zip(firsts, sizes)):
        copies.append(
            [
                pltpu.make_async_copy(
                    source.at[pl.ds(first * size, count * size), :], buf.at[pl.ds(first * size, count * size), :], sems.at[kind, n]
                )
                for kind, (source, buf, size) in enumerate(
                    ((field_hbm, field_buf, BS), (main_hbm, main_buf, 6 * BS), (side_hbm, side_buf, 6 * BS))
                )
            ]
        )
    for n in range(AHEAD):
        for kind in range(3):
            copies[n][kind].start()
    perm_ref[...] = split_matrix(width).astype(BF16)
    first_row = lax.axis_index("depth") * (blocks * BS)

    def small_tables():
        zero_ends(start_ref)
        weight_ref[...] = jnp.dot(
            jnp.broadcast_to(coupling_buf[...], (8, width)),
            split_matrix(width),
            preferred_element_type=F32,
            precision=lax.Precision.HIGHEST,
        )
        shape = floor_ref.shape
        floors = jnp.zeros(shape, jnp.int32)
        for step in range(STEPS):
            floors = jnp.where(lax.broadcasted_iota(jnp.int32, shape, 0) == step, floors_buf[step] - first_row, floors)
        floor_ref[...] = floors
        local = receivers_buf[...] - first_row
        local = jnp.where(jnp.logical_and(local >= 0, local < blocks * BS), local, blocks * BS)
        mine = local.shape[0] // 2
        turned = jnp.concatenate([local[mine:], local[:mine]], axis=0)
        pick_ref[...] = jnp.where(lax.axis_index("depth") == 0, turned, local)

    def split_chunk(n):
        for b in range(firsts[n], firsts[n] + sizes[n]):
            field = jnp.dot(field_buf[b * BS : (b + 1) * BS, :], perm_ref[...], preferred_element_type=F32).astype(BF16)
            put_block(start_ref, b + 1, field)

    def order_block(b, kind):
        buf = (main_buf, side_buf)[kind]
        plane = planes.at[(b * 2 + kind) % planes.shape[0]]
        plane[...] = buf[b * BS * 6 : (b + 1) * BS * 6, :].astype(F32)
        for m in range(6):
            ordered_ref[b, m, kind * BS : (kind + 1) * BS, :] = plane[pl.ds(m, BS, stride=6), :].astype(BF16)

    for n in range(len(sizes)):
        for kind in range(3):
            copies[n][kind].wait()
            if n + AHEAD < len(sizes):
                copies[n + AHEAD][kind].start()
        split_chunk(n)
        for b in range(firsts[n], firsts[n] + sizes[n]):
            order_block(b, 0)
            order_block(b, 1)
        if n == 1:
            coupling_copy.wait()
            floors_copy.wait()
            receivers_copy.wait()
            small_tables()
    edge_at = pl.multiple_of((1 + (blocks - 1) * (1 - lax.axis_index("depth"))) * 2 * BS, 2 * BS)
    edge_ref[...] = jnp.concatenate([start_ref[0, pl.ds(edge_at, BS), :], start_ref[1, pl.ds(edge_at, BS), :]], axis=1)


def whole_step(step, last):
    def kernel(ordered_ref, field_ref, weight_ref, floor_ref, next_ref):
        blocks = ordered_ref.shape[0]
        floors = floor_ref[step : step + 1, :]
        weights = weight_ref[...]
        if last:
            next_ref[:, blocks * BS :, :] = jnp.zeros((2, next_ref.shape[1] - blocks * BS, next_ref.shape[2]), F32)
        else:
            zero_ends(next_ref)

        def put(b, product):
            field = finished(product, weights, b * BS, floors)
            if last:
                put_final(next_ref, b * BS, field)
            else:
                put_block(next_ref, b + 1, field)

        def rows_of(b, k):
            return jnp.concatenate([ordered_ref[b, 2 * k], ordered_ref[b, 2 * k + 1]], axis=1)

        opened, half_done = None, None
        for b in range(blocks):
            at = (b + 1) * 2 * BS
            readers = [r for r in (b + 1, b, b - 1) if 0 <= r < blocks]
            left = jnp.concatenate([rows_of(r, b - r + 1) for r in readers], axis=0)
            right = jnp.concatenate([field_ref[0, at : at + 2 * BS, :], field_ref[1, at : at + 2 * BS, :]], axis=1)
            product = jnp.dot(left, right, preferred_element_type=F32)
            part = {r: product[i * 2 * BS : (i + 1) * 2 * BS] for i, r in enumerate(readers)}
            if b > 0:
                put(b - 1, half_done + part[b - 1])
            half_done = part[b] if opened is None else opened + part[b]
            opened = part.get(b + 1)
        put(blocks - 1, half_done)

    return kernel


def edge_block(step, ordered_ref, field_ref, weight_ref, floor_ref, halo_ref, halo_buf):
    blocks = ordered_ref.shape[0]
    side = lax.axis_index("depth")
    halo = halo_ref[...]
    b = (blocks - 1) * (1 - side)
    size = 2 * BS
    at = pl.multiple_of(b * size, size)
    halo_buf[:, size : 2 * size, :] = field_ref[:, pl.ds(at + size, size), :]
    inner = pl.multiple_of(at + 2 * size * side, size)
    halo_buf[:, pl.ds(pl.multiple_of(2 * size * side, size), size), :] = field_ref[:, pl.ds(inner, size), :]
    put_block(halo_buf, 2 * (1 - side), halo)
    field = advanced(
        operator_rows(ordered_ref, b), three_blocks(halo_buf, 0), weight_ref[...], b * BS, floor_ref[step : step + 1, :]
    )
    return b, field


def edge_step(step):
    def kernel(ordered_ref, field_ref, weight_ref, floor_ref, halo_ref, in_ref, next_ref, out_ref, halo_buf):
        del in_ref
        b, field = edge_block(step, ordered_ref, field_ref, weight_ref, floor_ref, halo_ref, halo_buf)
        out_ref[...] = field
        put_block(next_ref, b + 1, field)

    return kernel


def edge_and_pick(
    ordered_ref, field_ref, weight_ref, floor_ref, halo_ref, in_ref, rows_vmem,
    final_ref, send_ref, halo_buf, picked, rows_ref, sem,
):
    del in_ref
    rows_copy = pltpu.make_async_copy(rows_vmem, rows_ref, sem)
    rows_copy.start()
    b, field = edge_block(STEPS - 1, ordered_ref, field_ref, weight_ref, floor_ref, halo_ref, halo_buf)
    put_final(final_ref, pl.multiple_of(b * BS, BS), field)
    rows_copy.wait()
    gather_rows(final_ref, rows_ref, 0, picked, send_ref)


def pick_own(final_ref, rows_vmem, keep_ref, picked, rows_ref, sem):
    rows_copy = pltpu.make_async_copy(rows_vmem, rows_ref, sem)
    rows_copy.start()
    rows_copy.wait()
    gather_rows(final_ref, rows_ref, keep_ref.shape[0], picked, keep_ref)


def gather_rows(final_ref, rows_ref, first, picked, out_ref):
    lanes = rows_ref.shape[1]
    for n in range(out_ref.shape[0]):
        at = rows_ref[(first + n) // lanes, (first + n) % lanes]
        for part in range(2):
            picked[part, n : n + 1, :] = final_ref[part, pl.ds(at, 1), :]
    out_ref[...] = jnp.concatenate([picked[0], picked[1]], axis=1).astype(BF16)


def basis_kernel(freq_ref, out_ref):
    core = lax.axis_index("core")
    spread = 32
    lanes = freq_ref.shape[1]
    chip = (lax.axis_index("x") * lax.axis_size("y") + lax.axis_index("y")) * lax.axis_size("zh") + lax.axis_index("zh")
    turn = 2.0 * math.pi

    def unit(count_times_freq):
        cycles = count_times_freq * (1.0 / NT)
        angle = turn * (cycles - jnp.floor(cycles))
        return jnp.cos(angle), jnp.sin(angle)

    sample = (core * spread + lax.broadcasted_iota(jnp.int32, (spread, lanes), 0)).astype(F32)
    state = []
    turns = []
    for which in (core, 1 - core):
        freq = jnp.broadcast_to(freq_ref[pl.ds(chip * 2 + which, 1), :], (spread, lanes))
        state += list(unit(freq * sample))
        turns.append(unit(freq * (2.0 * spread)))

    def some(q, state):
        at = pl.multiple_of(q * spread, spread)
        out = []
        for which in range(2):
            c, s = state[2 * which], state[2 * which + 1]
            tc, ts = turns[which]
            out_ref[pl.ds(at, spread), 2 * which * lanes : (2 * which + 1) * lanes] = c.astype(BF16)
            out_ref[pl.ds(at, spread), (2 * which + 1) * lanes : (2 * which + 2) * lanes] = (-s).astype(BF16)
            out += [c * tc - s * ts, s * tc + c * ts]
        return tuple(out)

    lax.fori_loop(0, NT // (2 * spread), some, tuple(state))


def series_kernel(basis_ref, keep_ref, got_ref, keep2_ref, got2_ref, out_ref):
    picked = jnp.concatenate([keep_ref[...] + got_ref[...], keep2_ref[...] + got2_ref[...]], axis=1)
    product = lax.dot_general(basis_ref[...], picked, (((1,), (1,)), ((), ())), preferred_element_type=F32)
    out_ref[...] = product.astype(BF16)


def local(pressure_field, block_main, block_coupled, coupling, frequencies, receivers, floors):
    rows, width = pressure_field.shape
    blocks = rows // BS
    swap = [(0, 1), (1, 0)]
    padded = (2, (blocks + 2) * 2 * BS, width // 2)
    halo_buf = pltpu.VMEM((2, 6 * BS, width // 2), BF16)
    ordered, start, edge, weights, floor_rows, pick_rows = pl.pallas_call(
        load,
        out_shape=(
            vmem((blocks, 6, 2 * BS, BS), BF16),
            vmem(padded, BF16),
            vmem((BS, width), BF16),
            vmem((8, width), F32),
            vmem((8, width // 2), jnp.int32),
            vmem((receivers.shape[0] // BS, BS), jnp.int32),
        ),
        in_specs=[HBM_SPEC] * 6,
        out_specs=(VMEM_SPEC,) * 6,
        scratch_shapes=[
            pltpu.VMEM((rows * 6, BS), BF16),
            pltpu.VMEM((rows * 6, BS), BF16),
            pltpu.VMEM((rows, width), BF16),
            pltpu.VMEM((16, BS * 6, BS), F32),
            pltpu.VMEM((width, width), BF16),
            pltpu.VMEM((1, width), F32),
            pltpu.SMEM((STEPS,), jnp.int32),
            pltpu.VMEM((receivers.shape[0] // BS, BS), jnp.int32),
            pltpu.SemaphoreType.DMA((3, len(CHUNKS))),
            pltpu.SemaphoreType.DMA((3,)),
        ],
        compiler_params=limit(28),
        name="load",
    )(
        in_hbm(block_main.reshape(rows * 6, BS)),
        in_hbm(block_coupled.reshape(rows * 6, BS)),
        in_hbm(pressure_field),
        in_hbm(coupling.reshape(1, width)),
        in_hbm(floors),
        in_hbm(receivers.reshape(-1, BS)),
    )

    before = start
    for step in range(STEPS):
        last = step == STEPS - 1
        halo = lax.ppermute(edge, "depth", swap)
        field = pl.pallas_call(
            whole_step(step, last),
            out_shape=vmem((2, rows + 8, width // 2), F32) if last else vmem(padded, BF16),
            in_specs=[VMEM_SPEC] * 4,
            out_specs=VMEM_SPEC,
            compiler_params=limit(6),
            name="whole_step",
        )(ordered, before, weights, floor_rows)
        if last:
            break
        before, edge = pl.pallas_call(
            edge_step(step),
            out_shape=(vmem(padded, BF16), vmem((BS, width), BF16)),
            in_specs=[VMEM_SPEC] * 6,
            out_specs=(VMEM_SPEC,) * 2,
            input_output_aliases={5: 0},
            scratch_shapes=[halo_buf],
            compiler_params=limit(6),
            name="edge_step",
        )(ordered, before, weights, floor_rows, halo, field)

    owned = receivers.shape[0] // lax.axis_size("depth")
    pick_scratch = [
        pltpu.VMEM((2, owned, width // 2), F32),
        pltpu.SMEM(pick_rows.shape, jnp.int32),
        pltpu.SemaphoreType.DMA,
    ]
    final, send = pl.pallas_call(
        edge_and_pick,
        out_shape=(vmem((2, rows + 8, width // 2), F32), vmem((owned, width), BF16)),
        in_specs=[VMEM_SPEC] * 7,
        out_specs=(VMEM_SPEC,) * 2,
        input_output_aliases={5: 0},
        scratch_shapes=[halo_buf] + pick_scratch,
        compiler_params=limit(6),
        name="edge_and_pick",
    )(ordered, before, weights, floor_rows, halo, field, pick_rows)

    got = lax.ppermute(send, "depth", swap)
    keep = pl.pallas_call(
        pick_own,
        out_shape=vmem((owned, width), BF16),
        in_specs=[VMEM_SPEC] * 2,
        out_specs=VMEM_SPEC,
        scratch_shapes=pick_scratch,
        compiler_params=limit(6),
        name="pick_own",
    )(final, pick_rows)
    keep2 = lax.ppermute(keep, "core", swap)
    basis = pl.pallas_call(
        basis_kernel,
        out_shape=vmem((NT // 2, 2 * width), BF16),
        in_specs=[VMEM_SPEC],
        out_specs=VMEM_SPEC,
        compiler_params=limit(8),
        name="basis",
    )(frequencies.reshape(-1, width // 2))
    got2 = lax.ppermute(got, "core", swap)
    partial = pl.pallas_call(
        series_kernel,
        out_shape=jax.ShapeDtypeStruct((NT // 2, owned), BF16),
        in_specs=[VMEM_SPEC] * 5,
        out_specs=VMEM_SPEC,
        compiler_params=limit(8),
        name="series",
    )(basis, keep, got, keep2, got2)
    others = ("x", "y", "zh")
    groups = lax.axis_size(others)
    arrived = lax.all_to_all(
        partial.reshape(groups, NT // 2 // groups, owned), others, split_axis=0, concat_axis=0, tiled=True
    )
    summed = arrived.astype(F32).sum(axis=0) * (1.0 / math.sqrt(frequencies.shape[0]))
    return summed.T


def solution(mesh):
    chips = Mesh(mesh.devices.reshape(4, 4, 2, 2, 2), ("x", "y", "zh", "core", "depth"))
    freq = ("x", "y", "zh", "core")
    in_specs = (
        P("depth", freq),
        P("depth", None, None, None),
        P("depth", None, None, None),
        P(freq),
        P(),
        P(),
        P(),
    )

    return jax.shard_map(local, mesh=chips, in_specs=in_specs, out_specs=P("depth", freq), check_vma=False)
```

```python
import functools
import math

import jax
import jax.numpy as jnp
from jax import lax
from jax.experimental import pallas as pl
from jax.experimental.pallas import tpu as pltpu
from jax.sharding import Mesh, PartitionSpec as P


NT = 2048
STEPS = 4
BS = 128
F32 = jnp.float32
BF16 = jnp.bfloat16
CHUNKS = (1, 3, 4, 4, 4, 4, 4, 4, 2, 2)
AHEAD = 3

VMEM_SPEC = pl.BlockSpec(memory_space=pltpu.VMEM)
HBM_SPEC = pl.BlockSpec(memory_space=pl.ANY)


def limit(mebibytes):
    return pltpu.CompilerParams(vmem_limit_bytes=mebibytes << 20)


def in_hbm(x):
    return pltpu.with_memory_space_constraint(x, pltpu.HBM)


def vmem(shape, dtype):
    return pltpu.VMEM(shape, dtype)


def split_matrix(width):
    half = width // 2
    source = lax.broadcasted_iota(jnp.int32, (width, width), 0)
    target = lax.broadcasted_iota(jnp.int32, (width, width), 1)
    return jnp.where(source == 2 * (target % half) + target // half, 1.0, 0.0).astype(F32)


def put_block(ref, b, field):
    half = field.shape[1] // 2
    at = b * (2 * BS)
    if not isinstance(at, int):
        at = pl.multiple_of(at, 2 * BS)
    real = field[:, :half]
    imag = field[:, half:]
    ref[0, pl.ds(at, BS), :] = real
    ref[1, pl.ds(at, BS), :] = imag
    ref[0, pl.ds(at + BS, BS), :] = -imag
    ref[1, pl.ds(at + BS, BS), :] = real


def three_blocks(ref, b):
    at = b * (2 * BS)
    if not isinstance(at, int):
        at = pl.multiple_of(at, 2 * BS)
    return jnp.concatenate([ref[0, pl.ds(at, 6 * BS), :], ref[1, pl.ds(at, 6 * BS), :]], axis=1)


def operator_rows(ordered_ref, b):
    return jnp.concatenate([ordered_ref[b, m] for m in range(ordered_ref.shape[1])], axis=1)


def advanced(ordered, stacked, weights, first_row, floor_rows):
    return finished(jnp.dot(ordered, stacked, preferred_element_type=F32), weights, first_row, floor_rows)


def finished(product, weights, first_row, floor_rows):
    size = product.shape[0] // 2
    half = product.shape[1] // 2
    wr = weights[0:1, :half]
    wi = weights[0:1, half:]
    side_real = product[size:, :half]
    side_imag = product[size:, half:]
    real = product[:size, :half] + (wr * side_real - wi * side_imag)
    imag = product[:size, half:] + (wr * side_imag + wi * side_real)
    row = first_row + lax.broadcasted_iota(jnp.int32, (size, half), 0)
    damping = jnp.where(row >= floor_rows, 0.5, 1.0).astype(F32)
    return jnp.concatenate([damping * real, damping * imag], axis=1).astype(BF16)


def put_final(ref, at, field):
    half = field.shape[1] // 2
    ref[0, pl.ds(at, BS), :] = field[:, :half].astype(F32)
    ref[1, pl.ds(at, BS), :] = field[:, half:].astype(F32)


def zero_ends(ref):
    edge = jnp.zeros((2, 2 * BS, ref.shape[2]), ref.dtype)
    ref[:, 0 : 2 * BS, :] = edge
    ref[:, ref.shape[1] - 2 * BS :, :] = edge


def chunk_sizes(blocks):
    return [part * blocks // sum(CHUNKS) for part in CHUNKS]


def load(
    main_hbm, side_hbm, field_hbm, coupling_hbm, floors_hbm,
    receivers_hbm, ordered_ref, start_ref, edge_ref, weight_ref, floor_ref, pick_ref,
    main_buf, side_buf, field_buf, planes, perm_ref, coupling_buf, floors_buf, receivers_buf, sems, small_sems,
):
    blocks = ordered_ref.shape[0]
    sizes = chunk_sizes(blocks)
    firsts = [sum(sizes[:n]) for n in range(len(sizes))]
    width = field_buf.shape[1]
    coupling_copy = pltpu.make_async_copy(coupling_hbm, coupling_buf, small_sems.at[0])
    floors_copy = pltpu.make_async_copy(floors_hbm, floors_buf, small_sems.at[1])
    receivers_copy = pltpu.make_async_copy(receivers_hbm, receivers_buf, small_sems.at[2])
    coupling_copy.start()
    floors_copy.start()
    receivers_copy.start()
    copies = []
    for n, (first, count) in enumerate(zip(firsts, sizes)):
        copies.append(
            [
                pltpu.make_async_copy(
                    source.at[pl.ds(first * size, count * size), :], buf.at[pl.ds(first * size, count * size), :], sems.at[kind, n]
                )
                for kind, (source, buf, size) in enumerate(
                    ((field_hbm, field_buf, BS), (main_hbm, main_buf, 6 * BS), (side_hbm, side_buf, 6 * BS))
                )
            ]
        )
    for n in range(AHEAD):
        for kind in range(3):
            copies[n][kind].start()
    perm_ref[...] = split_matrix(width).astype(BF16)
    first_row = lax.axis_index("depth") * (blocks * BS)

    def small_tables():
        zero_ends(start_ref)
        weight_ref[...] = jnp.dot(
            jnp.broadcast_to(coupling_buf[...], (8, width)),
            split_matrix(width),
            preferred_element_type=F32,
            precision=lax.Precision.HIGHEST,
        )
        shape = floor_ref.shape
        floors = jnp.zeros(shape, jnp.int32)
        for step in range(STEPS):
            floors = jnp.where(lax.broadcasted_iota(jnp.int32, shape, 0) == step, floors_buf[step] - first_row, floors)
        floor_ref[...] = floors
        local = receivers_buf[...] - first_row
        local = jnp.where(jnp.logical_and(local >= 0, local < blocks * BS), local, blocks * BS)
        mine = local.shape[0] // 2
        turned = jnp.concatenate([local[mine:], local[:mine]], axis=0)
        pick_ref[...] = jnp.where(lax.axis_index("depth") == 0, turned, local)

    def split_chunk(n):
        for b in range(firsts[n], firsts[n] + sizes[n]):
            field = jnp.dot(field_buf[b * BS : (b + 1) * BS, :], perm_ref[...], preferred_element_type=F32).astype(BF16)
            put_block(start_ref, b + 1, field)

    def order_block(b, kind):
        buf = (main_buf, side_buf)[kind]
        plane = planes.at[(b * 2 + kind) % planes.shape[0]]
        plane[...] = buf[b * BS * 6 : (b + 1) * BS * 6, :].astype(F32)
        for m in range(6):
            ordered_ref[b, m, kind * BS : (kind + 1) * BS, :] = plane[pl.ds(m, BS, stride=6), :].astype(BF16)

    for n in range(len(sizes)):
        for kind in range(3):
            copies[n][kind].wait()
            if n + AHEAD < len(sizes):
                copies[n + AHEAD][kind].start()
        split_chunk(n)
        for b in range(firsts[n], firsts[n] + sizes[n]):
            order_block(b, 0)
            order_block(b, 1)
        if n == 1:
            coupling_copy.wait()
            floors_copy.wait()
            receivers_copy.wait()
            small_tables()
    edge_at = pl.multiple_of((1 + (blocks - 1) * (1 - lax.axis_index("depth"))) * 2 * BS, 2 * BS)
    edge_ref[...] = jnp.concatenate([start_ref[0, pl.ds(edge_at, BS), :], start_ref[1, pl.ds(edge_at, BS), :]], axis=1)


def whole_step(step, last):
    def kernel(ordered_ref, field_ref, weight_ref, floor_ref, next_ref):
        blocks = ordered_ref.shape[0]
        floors = floor_ref[step : step + 1, :]
        weights = weight_ref[...]
        if last:
            next_ref[:, blocks * BS :, :] = jnp.zeros((2, next_ref.shape[1] - blocks * BS, next_ref.shape[2]), F32)
        else:
            zero_ends(next_ref)

        def put(b, product):
            field = finished(product, weights, b * BS, floors)
            if last:
                put_final(next_ref, b * BS, field)
            else:
                put_block(next_ref, b + 1, field)

        def rows_of(b, k):
            return jnp.concatenate([ordered_ref[b, 2 * k], ordered_ref[b, 2 * k + 1]], axis=1)

        opened, half_done = None, None
        for b in range(blocks):
            at = (b + 1) * 2 * BS
            readers = [r for r in (b + 1, b, b - 1) if 0 <= r < blocks]
            left = jnp.concatenate([rows_of(r, b - r + 1) for r in readers], axis=0)
            right = jnp.concatenate([field_ref[0, at : at + 2 * BS, :], field_ref[1, at : at + 2 * BS, :]], axis=1)
            product = jnp.dot(left, right, preferred_element_type=F32)
            part = {r: product[i * 2 * BS : (i + 1) * 2 * BS] for i, r in enumerate(readers)}
            if b > 0:
                put(b - 1, half_done + part[b - 1])
            half_done = part[b] if opened is None else opened + part[b]
            opened = part.get(b + 1)
        put(blocks - 1, half_done)

    return kernel


def edge_block(step, ordered_ref, field_ref, weight_ref, floor_ref, halo_ref, halo_buf):
    blocks = ordered_ref.shape[0]
    side = lax.axis_index("depth")
    halo = halo_ref[...]
    b = (blocks - 1) * (1 - side)
    size = 2 * BS
    at = pl.multiple_of(b * size, size)
    halo_buf[:, size : 2 * size, :] = field_ref[:, pl.ds(at + size, size), :]
    inner = pl.multiple_of(at + 2 * size * side, size)
    halo_buf[:, pl.ds(pl.multiple_of(2 * size * side, size), size), :] = field_ref[:, pl.ds(inner, size), :]
    put_block(halo_buf, 2 * (1 - side), halo)
    field = advanced(
        operator_rows(ordered_ref, b), three_blocks(halo_buf, 0), weight_ref[...], b * BS, floor_ref[step : step + 1, :]
    )
    return b, field


def edge_step(step):
    def kernel(ordered_ref, field_ref, weight_ref, floor_ref, halo_ref, in_ref, next_ref, out_ref, halo_buf):
        del in_ref
        b, field = edge_block(step, ordered_ref, field_ref, weight_ref, floor_ref, halo_ref, halo_buf)
        out_ref[...] = field
        put_block(next_ref, b + 1, field)

    return kernel


def edge_and_pick(
    ordered_ref, field_ref, weight_ref, floor_ref, halo_ref, in_ref, rows_vmem,
    final_ref, send_ref, halo_buf, picked, rows_ref, sem,
):
    del in_ref
    rows_copy = pltpu.make_async_copy(rows_vmem, rows_ref, sem)
    rows_copy.start()
    b, field = edge_block(STEPS - 1, ordered_ref, field_ref, weight_ref, floor_ref, halo_ref, halo_buf)
    put_final(final_ref, pl.multiple_of(b * BS, BS), field)
    rows_copy.wait()
    gather_rows(final_ref, rows_ref, 0, picked, send_ref)


def pick_own(final_ref, rows_vmem, keep_ref, picked, rows_ref, sem):
    rows_copy = pltpu.make_async_copy(rows_vmem, rows_ref, sem)
    rows_copy.start()
    rows_copy.wait()
    gather_rows(final_ref, rows_ref, keep_ref.shape[0], picked, keep_ref)


def gather_rows(final_ref, rows_ref, first, picked, out_ref):
    lanes = rows_ref.shape[1]
    for n in range(out_ref.shape[0]):
        at = rows_ref[(first + n) // lanes, (first + n) % lanes]
        for part in range(2):
            picked[part, n : n + 1, :] = final_ref[part, pl.ds(at, 1), :]
    out_ref[...] = jnp.concatenate([picked[0], picked[1]], axis=1).astype(BF16)


def basis_kernel(freq_ref, out_ref):
    core = lax.axis_index("core")
    spread = 32
    lanes = freq_ref.shape[1]
    chip = (lax.axis_index("x") * lax.axis_size("y") + lax.axis_index("y")) * lax.axis_size("zh") + lax.axis_index("zh")
    turn = 2.0 * math.pi

    def unit(count_times_freq):
        cycles = count_times_freq * (1.0 / NT)
        angle = turn * (cycles - jnp.floor(cycles))
        return jnp.cos(angle), jnp.sin(angle)

    sample = (core * spread + lax.broadcasted_iota(jnp.int32, (spread, lanes), 0)).astype(F32)
    state = []
    turns = []
    for which in (core, 1 - core):
        freq = jnp.broadcast_to(freq_ref[pl.ds(chip * 2 + which, 1), :], (spread, lanes))
        state += list(unit(freq * sample))
        turns.append(unit(freq * (2.0 * spread)))

    def some(q, state):
        at = pl.multiple_of(q * spread, spread)
        out = []
        for which in range(2):
            c, s = state[2 * which], state[2 * which + 1]
            tc, ts = turns[which]
            out_ref[pl.ds(at, spread), 2 * which * lanes : (2 * which + 1) * lanes] = c.astype(BF16)
            out_ref[pl.ds(at, spread), (2 * which + 1) * lanes : (2 * which + 2) * lanes] = (-s).astype(BF16)
            out += [c * tc - s * ts, s * tc + c * ts]
        return tuple(out)

    lax.fori_loop(0, NT // (2 * spread), some, tuple(state))


def series_kernel(factor, basis_ref, keep_ref, got_ref, keep2_ref, got2_ref, out_ref):
    picked = jnp.concatenate([keep_ref[...] + got_ref[...], keep2_ref[...] + got2_ref[...]], axis=1)
    product = lax.dot_general(basis_ref[...], picked, (((1,), (1,)), ((), ())), preferred_element_type=F32)
    out_ref[...] = (product * factor).astype(BF16)


def local(pressure_field, block_main, block_coupled, coupling, frequencies, receivers, floors):
    rows, width = pressure_field.shape
    blocks = rows // BS
    swap = [(0, 1), (1, 0)]
    padded = (2, (blocks + 2) * 2 * BS, width // 2)
    halo_buf = pltpu.VMEM((2, 6 * BS, width // 2), BF16)
    ordered, start, edge, weights, floor_rows, pick_rows = pl.pallas_call(
        load,
        out_shape=(
            vmem((blocks, 6, 2 * BS, BS), BF16),
            vmem(padded, BF16),
            vmem((BS, width), BF16),
            vmem((8, width), F32),
            vmem((8, width // 2), jnp.int32),
            vmem((receivers.shape[0] // BS, BS), jnp.int32),
        ),
        in_specs=[HBM_SPEC] * 6,
        out_specs=(VMEM_SPEC,) * 6,
        scratch_shapes=[
            pltpu.VMEM((rows * 6, BS), BF16),
            pltpu.VMEM((rows * 6, BS), BF16),
            pltpu.VMEM((rows, width), BF16),
            pltpu.VMEM((16, BS * 6, BS), F32),
            pltpu.VMEM((width, width), BF16),
            pltpu.VMEM((1, width), F32),
            pltpu.SMEM((STEPS,), jnp.int32),
            pltpu.VMEM((receivers.shape[0] // BS, BS), jnp.int32),
            pltpu.SemaphoreType.DMA((3, len(CHUNKS))),
            pltpu.SemaphoreType.DMA((3,)),
        ],
        compiler_params=limit(28),
        name="load",
    )(
        in_hbm(block_main.reshape(rows * 6, BS)),
        in_hbm(block_coupled.reshape(rows * 6, BS)),
        in_hbm(pressure_field),
        in_hbm(coupling.reshape(1, width)),
        in_hbm(floors),
        in_hbm(receivers.reshape(-1, BS)),
    )

    before = start
    for step in range(STEPS):
        last = step == STEPS - 1
        halo = lax.ppermute(edge, "depth", swap)
        field = pl.pallas_call(
            whole_step(step, last),
            out_shape=vmem((2, rows + 8, width // 2), F32) if last else vmem(padded, BF16),
            in_specs=[VMEM_SPEC] * 4,
            out_specs=VMEM_SPEC,
            compiler_params=limit(6),
            name="whole_step",
        )(ordered, before, weights, floor_rows)
        if last:
            break
        before, edge = pl.pallas_call(
            edge_step(step),
            out_shape=(vmem(padded, BF16), vmem((BS, width), BF16)),
            in_specs=[VMEM_SPEC] * 6,
            out_specs=(VMEM_SPEC,) * 2,
            input_output_aliases={5: 0},
            scratch_shapes=[halo_buf],
            compiler_params=limit(6),
            name="edge_step",
        )(ordered, before, weights, floor_rows, halo, field)

    owned = receivers.shape[0] // lax.axis_size("depth")
    pick_scratch = [
        pltpu.VMEM((2, owned, width // 2), F32),
        pltpu.SMEM(pick_rows.shape, jnp.int32),
        pltpu.SemaphoreType.DMA,
    ]
    final, send = pl.pallas_call(
        edge_and_pick,
        out_shape=(vmem((2, rows + 8, width // 2), F32), vmem((owned, width), BF16)),
        in_specs=[VMEM_SPEC] * 7,
        out_specs=(VMEM_SPEC,) * 2,
        input_output_aliases={5: 0},
        scratch_shapes=[halo_buf] + pick_scratch,
        compiler_params=limit(6),
        name="edge_and_pick",
    )(ordered, before, weights, floor_rows, halo, field, pick_rows)

    got = lax.ppermute(send, "depth", swap)
    keep = pl.pallas_call(
        pick_own,
        out_shape=vmem((owned, width), BF16),
        in_specs=[VMEM_SPEC] * 2,
        out_specs=VMEM_SPEC,
        scratch_shapes=pick_scratch,
        compiler_params=limit(6),
        name="pick_own",
    )(final, pick_rows)
    keep2 = lax.ppermute(keep, "core", swap)
    basis = pl.pallas_call(
        basis_kernel,
        out_shape=vmem((NT // 2, 2 * width), BF16),
        in_specs=[VMEM_SPEC],
        out_specs=VMEM_SPEC,
        compiler_params=limit(8),
        name="basis",
    )(frequencies.reshape(-1, width // 2))
    got2 = lax.ppermute(got, "core", swap)
    partial = pl.pallas_call(
        functools.partial(series_kernel, 1.0 / math.sqrt(frequencies.shape[0])),
        out_shape=jax.ShapeDtypeStruct((NT // 2, owned), BF16),
        in_specs=[VMEM_SPEC] * 5,
        out_specs=VMEM_SPEC,
        compiler_params=limit(8),
        name="series",
    )(basis, keep, got, keep2, got2)
    others = ("x", "y", "zh")
    groups = lax.axis_size(others)
    arrived = lax.all_to_all(
        partial.reshape(groups, NT // 2 // groups, owned), others, split_axis=0, concat_axis=0, tiled=True
    )
    return arrived.astype(F32).sum(axis=0).T


def solution(mesh):
    chips = Mesh(mesh.devices.reshape(4, 4, 2, 2, 2), ("x", "y", "zh", "core", "depth"))
    freq = ("x", "y", "zh", "core")
    in_specs = (
        P("depth", freq),
        P("depth", None, None, None),
        P("depth", None, None, None),
        P(freq),
        P(),
        P(),
        P(),
    )

    return jax.shard_map(local, mesh=chips, in_specs=in_specs, out_specs=P("depth", freq), check_vma=False)
```
